32 devices in a mesh: real: 2 (over y), env: 4 (over z), mpo: 2 (over x), col: 2 (over core).
Axes of the slice: x: 2, y: 2, z: 4, core: 2. Of those that a mesh axis runs over, the one named last changes fastest.
Arguments:
- held: bfloat16 [3072, 8, 384], P(('real', 'env', 'col')), parts along dimension 0, may hold values from -0.15625 to 0.15625
- owner_map: int32 [8, 192], P('real'), parts along dimension 0, may hold values from 0 to 1535, as said below
- kept: int32 [8], P(('real', 'env')), parts along dimension 0, may hold values from 96 to 384
- left_env: bfloat16 [14, 8, 384, 384], P('mpo', ('real', 'env')), parts along dimension 1, may hold values from -6 to 6
- mpo_tensor: float32 [14, 14, 4, 4], replicated, may hold values from -1 to 1
- mpo_mask: int32 [14, 14], replicated, may hold values 0 or 1
- fields: float32 [4], P('real'), parts along dimension 0, may hold values from -2 to 2
Outputs:
- new_env: float32 [14, 8, 384, 384], P('mpo', ('real', 'env'), None, 'col'), parts along dimension 1
The draws below stay inside these ranges and needn't reach their ends.
There are 2 independent parts, one for each index of `real`. The reference program is written for one: setup_inputs(seed, part) draws one part's arguments, and reference() takes and returns one part's arrays. A program takes and returns all parts, laid end to end along the dimension named above; an argument that names none is the same for every part. Nothing has to cross between parts.
Inputs may be any that keep to these rules, and one draw needn't show every extreme that they name: owner_map[t, j] is the slot of held that holds tile j of sector t; all entries differ. The owner of index o along env+col holds the slots o * 192 to (o + 1) * 192 - 1. Among the tiles of one sector (the sector of one env index), one owner holds at most 48, and for every sector some owner holds exactly 48.
All inputs are finite; a program needn't handle non-finite values.
Results may differ from the reference program's by a relative error of at most 0.0042.
Values may be sent and summed in bfloat16 or wider, within the bound.
A program may use at most 64 MiB of HBM per device.

```python
import jax
import jax.numpy as jnp
from jax import lax

P_SIZE = 4
K = 14
B = 384
TILE = 8
SEC_DEV = 1
S = 4
NT = 192
CAP = 48
POOL = 192
SLOTS = 1536
KSL = 7
KP = 14
N_MPO = 2


def draw_owner_map(key, part):
    owners = 2 * SEC_DEV * NT // CAP
    row_count = S // SEC_DEV
    tiles_row = SEC_DEV * NT
    heavy = jax.random.randint(jax.random.fold_in(key, 11), (owners,), 0, 4)
    order = jax.vmap(lambda sub: jax.random.permutation(sub, POOL))(jax.random.split(jax.random.fold_in(key, 12), owners))

    def one_row(row):
        row_key = jax.random.fold_in(jax.random.fold_in(key, 13), row)
        candidate = jnp.arange(owners * CAP, dtype=jnp.int32)
        cand_owner = candidate // CAP
        noise = jax.random.randint(jax.random.fold_in(row_key, 1), (owners * CAP,), 0, 4096)
        forced = jax.random.randint(jax.random.fold_in(row_key, 2), (), 0, owners)
        score = noise + heavy[cand_owner] * 2048 + jnp.where(cand_owner == forced, 32768, 0)
        score = score * (owners * CAP) + candidate
        unused, chosen = lax.top_k(score, tiles_row)
        chosen = jax.random.permutation(jax.random.fold_in(row_key, 3), chosen)
        chosen_owner = chosen // CAP
        chosen_rank = chosen % CAP
        position = order[chosen_owner, row * CAP + chosen_rank]
        return chosen_owner * POOL + position
    table = jax.vmap(one_row)(jnp.arange(row_count, dtype=jnp.int32))
    return table.reshape(S, NT).astype(jnp.int32)


def with_ends(drawn, key, least, largest):
    longest = drawn.shape.index(max(drawn.shape))
    spots = []
    for shift in (0, 1):
        where = [jax.random.randint(jax.random.fold_in(key, axis), (), 0, length) for axis, length in enumerate(drawn.shape)]
        where[longest] = (where[longest] + shift) % drawn.shape[longest]
        spots.append(tuple(where))
    return drawn.at[spots[0]].set(least).at[spots[1]].set(largest)


def block_scale(stream_key, shape, shards, smallest, top_value):
    factor_of = 1.0
    for axis_at, blocks in shards:
        steps = jax.random.uniform(jax.random.fold_in(jax.random.fold_in(stream_key, 6), axis_at), (blocks,), jnp.float32, smallest / len(shards), top_value / len(shards))
        factor_of = factor_of * jnp.repeat(jnp.exp(steps), shape[axis_at] // blocks).reshape((-1,) + (1,) * (len(shape) - 1 - axis_at))
    return factor_of


def bell_draw(own_key, dims, width, limit, pieces=(), held_as=jnp.bfloat16):
    drawn = width * jax.random.normal(own_key, dims, jnp.float32)
    if pieces:
        drawn = drawn * block_scale(own_key, dims, pieces, -0.22, 0.18)
    return jnp.clip(drawn, -limit, limit).astype(held_as)


def setup_inputs(seed: int = 0, part: int = 0) -> dict:
    splits = jax.random.split(jax.random.key(seed), 8)
    own_keys = jax.random.split(jax.random.fold_in(splits[7], part), 8)
    return {
        "held": bell_draw(own_keys[0], (SLOTS, TILE, B), (P_SIZE * B) ** -0.5, 0.15625, ((0, 8),)),
        "owner_map": draw_owner_map(jax.random.fold_in(jax.random.fold_in(splits[7], part), 71), part),
        "kept": with_ends(jax.random.randint(own_keys[2], (S,), B // 4, B + 1), jax.random.fold_in(own_keys[2], 1), B // 4, B).astype(jnp.int32),
        "left_env": bell_draw(own_keys[3], (KP, S, B, B), 1.0, 6.0, ((0, 2), (1, 4))),
        "mpo_tensor": bell_draw(splits[4], (K, K, P_SIZE, P_SIZE), (K * P_SIZE // 2) ** -0.5, 1.0, (), jnp.float32),
        "mpo_mask": with_ends((jax.random.randint(splits[5], (K, K), 0, 2) < 1).astype(jnp.int32), jax.random.fold_in(splits[5], 1), 0, 1),
        "fields": jnp.clip(jax.random.uniform(own_keys[6], (2,), jnp.float32, -2.0, 2.0), -2.0, 2.0),
    }


def build_couplings(mpo_tensor, mpo_mask, fields, padded):
    bond = mpo_tensor.shape[0]
    states = mpo_tensor.shape[2]
    base = mpo_tensor * mpo_mask.astype(jnp.float32)[:, :, None, None]
    level = jnp.arange(states, dtype=jnp.int32)
    spin_first = 0.5 - (level // 2).astype(jnp.float32)
    spin_second = 0.5 - (level % 2).astype(jnp.float32)
    onsite = jnp.diag(fields[0] * spin_first + fields[1] * spin_second)
    bond_index = jnp.arange(bond, dtype=jnp.int32)
    corner = (bond_index[:, None] == bond - 1) & (bond_index[None, :] == 0)
    base = base + jnp.where(corner[:, :, None, None], onsite[None, None, :, :], jnp.float32(0.0))
    return jnp.pad(base, ((0, padded - bond), (0, padded - bond), (0, 0), (0, 0)))


def reference(held, owner_map, kept, left_env, mpo_tensor, mpo_mask, fields):
    tiles = jnp.take(held, owner_map.reshape(-1), axis=0)
    sector_matrices = tiles.reshape(S, P_SIZE, B, B)
    columns = jnp.arange(B, dtype=jnp.int32)
    keep = columns[None, :] < kept[:, None]
    sector_matrices = jnp.where(keep[:, None, None, :], sector_matrices, jnp.zeros((), jnp.bfloat16))
    couplings = build_couplings(mpo_tensor, mpo_mask, fields, KP)
    leading_sector = lax.Precision.HIGHEST

    def one_sector(pair):
        block, environment = pair
        bond_vectors = block.astype(jnp.float32)
        first = jnp.einsum("wij,sja->wsia", environment[:K].astype(jnp.float32), bond_vectors, precision=leading_sector)
        contracted_sum = jnp.zeros((K, P_SIZE, B, B), jnp.float32)
        for slab_index in range(N_MPO):
            lower = slab_index * KSL
            upper = min(lower + KSL, K)
            if lower < K:
                next_spin = jnp.einsum("wvts,wsia->vtia", couplings[lower:upper, :K], first[lower:upper], precision=leading_sector)
                rounded = lax.optimization_barrier(next_spin.astype(jnp.bfloat16))
                contracted_sum = contracted_sum + rounded.astype(jnp.float32)
        updated_environment = jnp.einsum("hze,shzo->seo", bond_vectors, contracted_sum, precision=leading_sector)
        return jnp.pad(updated_environment, ((0, KP - K), (0, 0), (0, 0)))

    stacked = lax.map(one_sector, (sector_matrices, jnp.moveaxis(left_env, 1, 0)))
    return jnp.moveaxis(stacked, 0, 1)
```

```python
import functools

import jax
import jax.numpy as jnp
from jax import lax
from jax.experimental import pallas as pl
from jax.experimental.pallas import tpu as pltpu
from jax.sharding import PartitionSpec as P

MESH = pl.DeviceIdType.MESH
LANES = 128
GROUP = 4
BF = jnp.bfloat16


def build_couplings(mpo_tensor, mpo_mask, fields, padded):
    bond = mpo_tensor.shape[0]
    states = mpo_tensor.shape[2]
    base = mpo_tensor * mpo_mask.astype(jnp.float32)[:, :, None, None]
    level = jnp.arange(states, dtype=jnp.int32)
    spin_first = 0.5 - (level // 2).astype(jnp.float32)
    spin_second = 0.5 - (level % 2).astype(jnp.float32)
    onsite = jnp.diag(fields[0] * spin_first + fields[1] * spin_second)
    bond_index = jnp.arange(bond, dtype=jnp.int32)
    corner = (bond_index[:, None] == bond - 1) & (bond_index[None, :] == 0)
    base = base + jnp.where(corner[:, :, None, None], onsite[None, None, :, :], jnp.float32(0.0))
    return jnp.pad(base, ((0, padded - bond), (0, padded - bond), (0, 0), (0, 0)))


def iota(shape, dim):
    return lax.broadcasted_iota(jnp.int32, shape, dim)


def one_hot(condition):
    return jnp.where(condition, jnp.float32(1), jnp.float32(0)).astype(BF)


def mm(a, b):
    return jnp.dot(a, b, preferred_element_type=jnp.float32)


def pack_kernel(cores, map_ref, held_ref, out_ref):
    pool = held_ref.shape[0]
    rows, tiles = map_ref.shape
    low = (lax.axis_index("env") * cores + lax.axis_index("col")) * pool

    def sector(t, carry):
        def step(j, count):
            slot = map_ref[t, j] - low
            mine = (slot >= 0) & (slot < pool)
            out_ref[t, count] = held_ref[jnp.where(mine, slot, 0)]
            return count + mine.astype(jnp.int32)

        lax.fori_loop(0, tiles, step, jnp.int32(0), unroll=8)
        return carry

    lax.fori_loop(0, rows, sector, jnp.int32(0))


def comm_kernel(
    sizes, pack_ref, left_ref, arrived_ref, other_ref,
    z_send, z_recv, f_send, f_recv, x_send, x_recv, g_send, g_recv, own_sem,
):
    envs, planes, cores = sizes
    env, plane, core = lax.axis_index("env"), lax.axis_index("mpo"), lax.axis_index("col")
    cap = arrived_ref.shape[1]
    slab = left_ref.shape[0]
    part = left_ref.shape[2] // cores
    mate = lax.rem(core + 1, cores)

    barrier = pltpu.get_barrier_semaphore()
    for d in range(1, envs):
        pl.semaphore_signal(
            barrier, inc=1, device_id={"env": lax.rem(env + d, envs)}, device_id_type=MESH
        )
    for d in range(1, planes):
        pl.semaphore_signal(
            barrier, inc=1, device_id={"mpo": lax.rem(plane + d, planes)}, device_id_type=MESH
        )
    pl.semaphore_signal(barrier, inc=1, device_id={"col": mate}, device_id_type=MESH)
    pl.semaphore_wait(barrier, envs + planes - 1)

    def z_copy(d):
        target = lax.rem(env + d, envs)
        return pltpu.make_async_remote_copy(
            src_ref=pack_ref.at[target, pl.ds(0, cap)],
            dst_ref=arrived_ref.at[env * cores + core],
            send_sem=z_send.at[d], recv_sem=z_recv.at[d],
            device_id={"env": target}, device_id_type=MESH,
        )

    def f_copy(d):
        source = lax.rem(env - d + envs, envs)
        block = arrived_ref.at[source * cores + core]
        return pltpu.make_async_remote_copy(
            src_ref=pack_ref.at[env, pl.ds(0, cap)] if d == 0 else block,
            dst_ref=block,
            send_sem=f_send.at[d], recv_sem=f_recv.at[d],
            device_id={"col": mate}, device_id_type=MESH,
        )

    def x_copy(d, w):
        rows = pl.ds(pl.multiple_of(core * part, part), part)
        return pltpu.make_async_remote_copy(
            src_ref=left_ref.at[w, 0, rows],
            dst_ref=other_ref.at[(planes - d - 1) * slab + w, rows],
            send_sem=x_send.at[d, w], recv_sem=x_recv.at[d, w],
            device_id={"mpo": lax.rem(plane + d, planes)}, device_id_type=MESH,
        )

    def g_copy(d, w):
        rows = pl.ds(pl.multiple_of(core * part, part), part)
        piece = other_ref.at[(planes - d - 1) * slab + w, rows]
        return pltpu.make_async_remote_copy(
            src_ref=piece, dst_ref=piece,
            send_sem=g_send.at[d, w], recv_sem=g_recv.at[d, w],
            device_id={"col": mate}, device_id_type=MESH,
        )

    own = pltpu.make_async_copy(
        pack_ref.at[env, pl.ds(0, cap)], arrived_ref.at[env * cores + core], own_sem
    )
    z_order = list(range(envs - 1, 0, -1))
    x_order = [(d, w) for w in range(slab) for d in range(1, planes)]
    for d in z_order:
        z_copy(d).start()
    for d, w in x_order:
        x_copy(d, w).start()
    own.start()
    f_copy(0).start()

    waits = [("z", d, (i + 1) / len(z_order)) for i, d in enumerate(z_order)]
    waits += [("x", item, (i + 1) / len(x_order)) for i, item in enumerate(x_order)]
    for kind, item, _ in sorted(waits, key=lambda entry: entry[2]):
        if kind == "z":
            z_copy(item).wait_recv()
            f_copy(item).start()
        else:
            x_copy(*item).wait_recv()
            g_copy(*item).start()
    own.wait()
    f_copy(0).wait()
    for d in z_order:
        z_copy(d).wait_send()
        f_copy(d).wait()
    for item in x_order:
        x_copy(*item).wait_send()
        g_copy(*item).wait()


def contract_kernel(
    cores, pool, map_ref, kept_ref, arrived_ref, left_ref, other_ref, coupling_ref,
    out_ref, count_ref, tiles_ref, own_ref, turned_ref, first_ref, second_ref,
):
    env, core = lax.axis_index("env"), lax.axis_index("col")
    owners, cap, tile, width = arrived_ref.shape
    tiles = map_ref.shape[1]
    states = tiles * tile // width
    slab = left_ref.shape[0]
    slots = slab + other_ref.shape[0]
    padded = coupling_ref.shape[1] // states
    share = width // cores
    lanes = own_ref.shape[2]

    for s in range(owners):
        count_ref[s] = 0

    def fetch(j, carry):
        source = lax.div(map_ref[env, j], jnp.int32(pool))
        rank = count_ref[source]
        count_ref[source] = rank + 1
        tiles_ref[pl.ds(pl.multiple_of(j * tile, tile), tile), :] = arrived_ref[
            source, rank
        ].astype(jnp.float32)
        return carry

    lax.fori_loop(0, tiles, fetch, jnp.int32(0), unroll=8)

    kept = kept_ref[0]
    blocks = [
        jnp.where(
            iota((width, width), 1) < kept, tiles_ref[pl.ds(s * width, width), :], 0.0
        ).astype(BF)
        for s in range(states)
    ]

    pick = one_hot(
        (iota((width, lanes), 0) == iota((width, lanes), 1) + core * share)
        & (iota((width, lanes), 1) < share)
    )
    for s in range(states):
        own_ref[s] = mm(blocks[s], pick).astype(BF)

    chunk = 256 // states
    span = chunk * states
    row, col = iota((span, span), 0), iota((span, span), 1)
    unit = states * GROUP
    moved = (
        lax.rem(lax.div(row, GROUP), states) * chunk
        + lax.div(row, unit) * GROUP
        + lax.rem(row, GROUP)
    )
    regroup = one_hot(col == moved)
    for h in range(width // chunk):
        stack = jnp.concatenate(
            [blocks[s][h * chunk : (h + 1) * chunk] for s in range(states)], axis=0
        )
        turned_ref[:, pl.ds(h * span, span)] = mm(regroup, stack).T.astype(BF)

    pairs = slab * states
    tall, wide = pairs * GROUP, states * GROUP * padded
    spread_rows = one_hot(lax.div(iota((tall, pairs), 0), GROUP) == iota((tall, pairs), 1))
    source, target = iota((states * padded, wide), 0), iota((states * padded, wide), 1)
    spread_columns = one_hot(
        (lax.div(source, padded) == lax.div(target, GROUP * padded))
        & (lax.rem(source, padded) == lax.rem(target, padded))
    )
    diagonal = lax.rem(iota((tall, wide), 0), GROUP) == lax.rem(
        lax.div(iota((tall, wide), 1), padded), GROUP
    )
    coupling = coupling_ref[...]
    high = coupling.astype(BF)
    low = (coupling - high.astype(jnp.float32)).astype(BF)
    both = []
    for piece in (high, low):
        spread = mm(mm(spread_rows, piece).astype(BF), spread_columns)
        both.append(jnp.where(diagonal, spread, 0.0).astype(BF))
    mixing = jnp.concatenate(both, axis=0)

    step = 16
    block_rows = step * padded
    row, col = iota((block_rows, block_rows), 0), iota((block_rows, block_rows), 1)
    interleave = one_hot(col == lax.rem(row, padded) * step + lax.div(row, padded))
    rows_chunk = first_ref.shape[1] // padded
    per_group = GROUP * padded

    def chunk_step(h, carry):
        pieces = []
        for b in range(rows_chunk // step):
            rows = pl.ds(pl.multiple_of(h * rows_chunk + b * step, step), step)
            stack = [left_ref[w, 0, rows, :] for w in range(slab)]
            stack += [other_ref[w, rows, :] for w in range(slots - slab)]
            if padded > slots:
                stack.append(jnp.zeros(((padded - slots) * step, width), BF))
            pieces.append(mm(interleave, jnp.concatenate(stack, axis=0)).astype(BF))
        environment = jnp.concatenate(pieces, axis=0)
        for s in range(states):
            first_ref[s] = mm(environment, own_ref[s]).astype(BF)
        for g in range(rows_chunk // GROUP):
            operand = jnp.concatenate(
                [first_ref[s, pl.ds(g * per_group, per_group), :] for s in range(states)], axis=0
            )
            mixed = mm(mixing, operand)
            mixed = (mixed[:tall] + mixed[tall:]).astype(BF)
            at = pl.multiple_of(h * (rows_chunk * states) + g * unit, unit)
            for v in range(slab):
                second_ref[v, pl.ds(at, unit), :] = mixed[v * unit : (v + 1) * unit]
        return carry

    lax.fori_loop(0, width // rows_chunk, chunk_step, jnp.int32(0))

    def close(v, carry):
        out_ref[v] = mm(turned_ref[...], second_ref[v]).T[:share]
        return carry

    lax.fori_loop(0, slab, close, jnp.int32(0))


def on_device(held, owner_map, kept, left_env, mpo_tensor, mpo_mask, fields):
    envs, cores, planes = (lax.axis_size(name) for name in ("env", "col", "mpo"))
    plane = lax.axis_index("mpo")
    pool, tile, width = held.shape
    rows, tiles = owner_map.shape
    states = tiles * tile // width
    cap = 2 * kept.shape[0] * tiles // (envs * cores)
    slab = left_env.shape[0]
    slots = slab * planes
    padded = -(-slots // 16) * 16
    share = width // cores
    lanes = -(-share // LANES) * LANES
    smem = pl.BlockSpec(memory_space=pltpu.SMEM)
    vmem = pl.BlockSpec(memory_space=pltpu.VMEM)
    anywhere = pl.BlockSpec(memory_space=pl.ANY)
    dma = pltpu.SemaphoreType.DMA

    packed = pl.pallas_call(
        functools.partial(pack_kernel, cores),
        out_shape=jax.ShapeDtypeStruct((rows, cap + 1, tile, width), BF),
        in_specs=[smem, vmem],
        out_specs=vmem,
        name="pack",
    )(owner_map, held)

    arrived, other = pl.pallas_call(
        functools.partial(comm_kernel, (envs, planes, cores)),
        out_shape=[
            jax.ShapeDtypeStruct((envs * cores, cap, tile, width), BF),
            jax.ShapeDtypeStruct((slots - slab, width, width), BF),
        ],
        in_specs=[anywhere, anywhere],
        out_specs=[anywhere, anywhere],
        scratch_shapes=[
            dma((envs,)), dma((envs,)), dma((envs,)), dma((envs,)),
            dma((planes, slab)), dma((planes, slab)), dma((planes, slab)), dma((planes, slab)),
            dma,
        ],
        compiler_params=pltpu.CompilerParams(collective_id=0, has_side_effects=True),
        name="exchange",
    )(packed, left_env)

    couplings = build_couplings(mpo_tensor, mpo_mask, fields, slots)
    couplings = lax.dynamic_slice_in_dim(couplings, plane * slab, slab, 1)
    couplings = jnp.concatenate([couplings, couplings], axis=0)
    couplings = lax.dynamic_slice_in_dim(couplings, plane * slab, slots, 0)
    couplings = jnp.pad(couplings, ((0, padded - slots), (0, 0), (0, 0), (0, 0)))
    couplings = couplings.transpose(1, 2, 3, 0).reshape(slab * states, states * padded)

    chunk_rows = 64 * padded
    result = pl.pallas_call(
        functools.partial(contract_kernel, cores, pool),
        out_shape=jax.ShapeDtypeStruct((slab, share, width), jnp.float32),
        in_specs=[smem, smem, vmem, vmem, vmem, vmem],
        out_specs=vmem,
        scratch_shapes=[
            pltpu.SMEM((envs * cores,), jnp.int32),
            pltpu.VMEM((tiles * tile, width), jnp.float32),
            pltpu.VMEM((states, width, lanes), BF),
            pltpu.VMEM((width, tiles * tile), BF),
            pltpu.VMEM((states, chunk_rows, lanes), BF),
            pltpu.VMEM((slab, tiles * tile, lanes), BF),
        ],
        compiler_params=pltpu.CompilerParams(vmem_limit_bytes=48 * 1024 * 1024),
        name="contract",
    )(owner_map, kept, arrived, left_env, other, couplings)
    return jnp.swapaxes(result, 1, 2)[:, None]


def solution(mesh):
    return jax.shard_map(
        on_device,
        mesh=mesh,
        in_specs=(
            P(("real", "env", "col"), None, None),
            P("real", None),
            P(("real", "env")),
            P("mpo", ("real", "env"), None, None),
            P(),
            P(),
            P("real"),
        ),
        out_specs=P("mpo", ("real", "env"), None, "col"),
        check_vma=False,
    )
```

```python
import functools

import jax
import jax.numpy as jnp
from jax import lax
from jax.experimental import pallas as pl
from jax.experimental.pallas import tpu as pltpu
from jax.sharding import PartitionSpec as P

MESH = pl.DeviceIdType.MESH
LANES = 128
GROUP = 4
BF = jnp.bfloat16


def iota(shape, dim):
    return lax.broadcasted_iota(jnp.int32, shape, dim)


def one_hot(condition):
    return jnp.where(condition, jnp.float32(1), jnp.float32(0)).astype(BF)


def mm(a, b):
    return jnp.dot(a, b, preferred_element_type=jnp.float32)


def list_kernel(cores, pool, map_ref, list_ref):
    rows, tiles = map_ref.shape
    low = (lax.axis_index("env") * cores + lax.axis_index("col")) * pool

    def sector(t, carry):
        def step(j, count):
            slot = map_ref[t, j] - low
            list_ref[t, count] = slot
            return count + ((slot >= 0) & (slot < pool)).astype(jnp.int32)

        lax.fori_loop(0, tiles, step, jnp.int32(0), unroll=16)
        return carry

    lax.fori_loop(0, rows, sector, jnp.int32(0))


def quotient(value, divisor, limit):
    for shift in range(8, 31):
        factor = -(-(1 << shift) // divisor)
        if limit * factor < 2**31 and (factor * divisor - (1 << shift)) * limit < 1 << shift:
            return lax.shift_right_logical(value * factor, jnp.int32(shift))
    return lax.div(value, jnp.int32(divisor))


def comm_kernel(
    sizes, list_ref, held_ref, left_ref, arrived_ref, other_ref, pool_ref, pack_ref,
    z_send, z_recv, f_send, f_recv, x_send, x_recv, g_send, g_recv, own_sem, pool_sem,
):
    envs, planes, cores = sizes
    env, plane, core = lax.axis_index("env"), lax.axis_index("mpo"), lax.axis_index("col")
    cap = arrived_ref.shape[1]
    slab = left_ref.shape[0]
    part = left_ref.shape[2] // cores
    mate = lax.rem(core + 1, cores)

    fill = pltpu.make_async_copy(held_ref, pool_ref, pool_sem)
    fill.start()
    barrier = pltpu.get_barrier_semaphore()
    for d in range(1, envs):
        pl.semaphore_signal(
            barrier, inc=1, device_id={"env": lax.rem(env + d, envs)}, device_id_type=MESH
        )
    for d in range(1, planes):
        pl.semaphore_signal(
            barrier, inc=1, device_id={"mpo": lax.rem(plane + d, planes)}, device_id_type=MESH
        )
    pl.semaphore_signal(barrier, inc=1, device_id={"col": mate}, device_id_type=MESH)
    pl.semaphore_wait(barrier, envs + planes - 1)

    def z_copy(d):
        target = lax.rem(env + d, envs)
        return pltpu.make_async_remote_copy(
            src_ref=pack_ref.at[d],
            dst_ref=arrived_ref.at[env * cores + core],
            send_sem=z_send.at[d], recv_sem=z_recv.at[d],
            device_id={"env": target}, device_id_type=MESH,
        )

    def f_copy(d):
        source = lax.rem(env - d + envs, envs)
        block = arrived_ref.at[source * cores + core]
        return pltpu.make_async_remote_copy(
            src_ref=pack_ref.at[0] if d == 0 else block,
            dst_ref=block,
            send_sem=f_send.at[d], recv_sem=f_recv.at[d],
            device_id={"col": mate}, device_id_type=MESH,
        )

    def x_copy(d, w):
        rows = pl.ds(pl.multiple_of(core * part, part), part)
        return pltpu.make_async_remote_copy(
            src_ref=left_ref.at[w, 0, rows],
            dst_ref=other_ref.at[(planes - d - 1) * slab + w, rows],
            send_sem=x_send.at[d, w], recv_sem=x_recv.at[d, w],
            device_id={"mpo": lax.rem(plane + d, planes)}, device_id_type=MESH,
        )

    def g_copy(d, w):
        rows = pl.ds(pl.multiple_of(core * part, part), part)
        piece = other_ref.at[(planes - d - 1) * slab + w, rows]
        return pltpu.make_async_remote_copy(
            src_ref=piece, dst_ref=piece,
            send_sem=g_send.at[d, w], recv_sem=g_recv.at[d, w],
            device_id={"col": mate}, device_id_type=MESH,
        )

    own = pltpu.make_async_copy(
        pack_ref.at[0], arrived_ref.at[env * cores + core], own_sem
    )
    z_order = list(range(envs - 1, 0, -1))
    x_order = [(d, w) for w in range(slab) for d in range(1, planes)]
    for d, w in x_order:
        x_copy(d, w).start()
    fill.wait()

    def gather(d):
        target = lax.rem(env + d, envs)

        def step(p, carry):
            slot = jnp.clip(list_ref[target, p], 0, pool_ref.shape[0] - 1)
            pack_ref[d, p] = pool_ref[slot]
            return carry

        lax.fori_loop(0, cap, step, jnp.int32(0), unroll=8 if cap % 8 == 0 else 1)

    for i, d in enumerate(z_order + [0]):
        gather(d)
        if i:
            z_copy(z_order[i - 1]).start()

    waits = [("z", d, (i + 1) / len(z_order)) for i, d in enumerate(z_order)]
    waits += [("x", item, (i + 1) / len(x_order)) for i, item in enumerate(x_order)]
    own_started = False
    for kind, item, _ in sorted(waits, key=lambda entry: entry[2]):
        if kind == "z":
            z_copy(item).wait_recv()
            f_copy(item).start()
        else:
            x_copy(*item).wait_recv()
            g_copy(*item).start()
        if not own_started:
            own_started = True
            own.start()
            f_copy(0).start()
    own.wait()
    f_copy(0).wait()
    for d in z_order:
        z_copy(d).wait_send()
        f_copy(d).wait()
    for item in x_order:
        x_copy(*item).wait_send()
        g_copy(*item).wait()


def contract_kernel(
    cores, pool, bond, map_ref, kept_ref, fields_ref, arrived_ref, left_ref, other_ref, coupling_ref,
    out_ref, count_ref, tiles_ref, own_ref, turned_ref, first_ref, second_ref,
):
    env, core = lax.axis_index("env"), lax.axis_index("col")
    owners, cap, tile, width = arrived_ref.shape
    tiles = map_ref.shape[1]
    states = tiles * tile // width
    slab = left_ref.shape[0]
    slots = slab + other_ref.shape[0]
    padded = coupling_ref.shape[1] // states
    share = width // cores
    lanes = own_ref.shape[2]

    for s in range(owners):
        count_ref[s] = 0

    def fetch(j, carry):
        source = quotient(map_ref[env, j], pool, pool * owners)
        rank = count_ref[source]
        count_ref[source] = rank + 1
        tiles_ref[pl.ds(pl.multiple_of(j * tile, tile), tile), :] = arrived_ref[
            source, rank
        ].astype(jnp.float32)
        return carry

    lax.fori_loop(0, tiles, fetch, jnp.int32(0), unroll=8)

    kept = kept_ref[0]
    blocks = [
        jnp.where(
            iota((width, width), 1) < kept, tiles_ref[pl.ds(s * width, width), :], 0.0
        ).astype(BF)
        for s in range(states)
    ]

    pick = one_hot(
        (iota((width, lanes), 0) == iota((width, lanes), 1) + core * share)
        & (iota((width, lanes), 1) < share)
    )
    for s in range(states):
        own_ref[s] = mm(blocks[s], pick).astype(BF)

    chunk = 256 // states
    span = chunk * states
    row, col = iota((span, span), 0), iota((span, span), 1)
    unit = states * GROUP
    moved = (
        lax.rem(lax.div(row, GROUP), states) * chunk
        + lax.div(row, unit) * GROUP
        + lax.rem(row, GROUP)
    )
    regroup = one_hot(col == moved)
    for h in range(width // chunk):
        stack = jnp.concatenate(
            [blocks[s][h * chunk : (h + 1) * chunk] for s in range(states)], axis=0
        )
        turned_ref[:, pl.ds(h * span, span)] = mm(regroup, stack).T.astype(BF)

    pairs = slab * states
    tall, wide = pairs * GROUP, states * GROUP * padded
    spread_rows = one_hot(lax.div(iota((tall, pairs), 0), GROUP) == iota((tall, pairs), 1))
    source, target = iota((states * padded, wide), 0), iota((states * padded, wide), 1)
    spread_columns = one_hot(
        (lax.div(source, padded) == lax.div(target, GROUP * padded))
        & (lax.rem(source, padded) == lax.rem(target, padded))
    )
    diagonal = lax.rem(iota((tall, wide), 0), GROUP) == lax.rem(
        lax.div(iota((tall, wide), 1), padded), GROUP
    )
    row, col = iota((pairs, states * padded), 0), iota((pairs, states * padded), 1)
    state, slot = lax.div(col, padded), lax.rem(col, padded)
    first_slot = lax.axis_index("mpo") * slab
    turn = jnp.where(first_slot + slot >= slots, slots, 0)
    corner = (
        (first_slot + lax.div(row, states) == 0)
        & (first_slot + slot - turn == bond - 1)
        & (slot < slots)
        & (lax.rem(row, states) == state)
    )
    onsite = fields_ref[0] * (0.5 - lax.div(state, 2).astype(jnp.float32)) + fields_ref[1] * (
        0.5 - lax.rem(state, 2).astype(jnp.float32)
    )
    coupling = coupling_ref[...] + jnp.where(corner, onsite, 0.0)
    high = coupling.astype(BF)
    low = (coupling - high.astype(jnp.float32)).astype(BF)
    both = []
    for piece in (high, low):
        spread = mm(mm(spread_rows, piece).astype(BF), spread_columns)
        both.append(jnp.where(diagonal, spread, 0.0).astype(BF))
    mixing = jnp.concatenate(both, axis=0)

    step = 16
    block_rows = step * padded
    row, col = iota((block_rows, block_rows), 0), iota((block_rows, block_rows), 1)
    interleave = one_hot(col == lax.rem(row, padded) * step + lax.div(row, padded))
    rows_chunk = first_ref.shape[1] // padded
    per_group = GROUP * padded

    def chunk_step(h, carry):
        pieces = []
        for b in range(rows_chunk // step):
            rows = pl.ds(pl.multiple_of(h * rows_chunk + b * step, step), step)
            stack = [left_ref[w, 0, rows, :] for w in range(slab)]
            stack += [other_ref[w, rows, :] for w in range(slots - slab)]
            if padded > slots:
                stack.append(jnp.zeros(((padded - slots) * step, width), BF))
            pieces.append(mm(interleave, jnp.concatenate(stack, axis=0)).astype(BF))
        environment = jnp.concatenate(pieces, axis=0)
        for s in range(states):
            first_ref[s] = mm(environment, own_ref[s]).astype(BF)
        for g in range(rows_chunk // GROUP):
            operand = jnp.concatenate(
                [first_ref[s, pl.ds(g * per_group, per_group), :] for s in range(states)], axis=0
            )
            mixed = mm(mixing, operand)
            mixed = (mixed[:tall] + mixed[tall:]).astype(BF)
            at = pl.multiple_of(h * (rows_chunk * states) + g * unit, unit)
            for v in range(slab):
                second_ref[v, pl.ds(at, unit), :] = mixed[v * unit : (v + 1) * unit]
        return carry

    lax.fori_loop(0, width // rows_chunk, chunk_step, jnp.int32(0))

    def close(v, carry):
        out_ref[v] = mm(turned_ref[...], second_ref[v]).T[:share]
        return carry

    lax.fori_loop(0, slab, close, jnp.int32(0))


def on_device(held, owner_map, kept, left_env, mpo_tensor, mpo_mask, fields):
    envs, cores, planes = (lax.axis_size(name) for name in ("env", "col", "mpo"))
    plane = lax.axis_index("mpo")
    pool, tile, width = held.shape
    rows, tiles = owner_map.shape
    states = tiles * tile // width
    cap = 2 * kept.shape[0] * tiles // (envs * cores)
    slab = left_env.shape[0]
    slots = slab * planes
    padded = -(-slots // 16) * 16
    share = width // cores
    lanes = -(-share // LANES) * LANES
    smem = pl.BlockSpec(memory_space=pltpu.SMEM)
    vmem = pl.BlockSpec(memory_space=pltpu.VMEM)
    anywhere = pl.BlockSpec(memory_space=pl.ANY)
    dma = pltpu.SemaphoreType.DMA

    slot_list = pl.pallas_call(
        functools.partial(list_kernel, cores, pool),
        out_shape=jax.ShapeDtypeStruct((rows, cap + 1), jnp.int32),
        in_specs=[smem],
        out_specs=smem,
        name="slots",
    )(owner_map)

    arrived, other = pl.pallas_call(
        functools.partial(comm_kernel, (envs, planes, cores)),
        out_shape=[
            jax.ShapeDtypeStruct((envs * cores, cap, tile, width), BF),
            jax.ShapeDtypeStruct((slots - slab, width, width), BF),
        ],
        in_specs=[smem, anywhere, anywhere],
        out_specs=[anywhere, anywhere],
        scratch_shapes=[
            pltpu.VMEM((pool, tile, width), BF),
            pltpu.VMEM((envs, cap, tile, width), BF),
            dma((envs,)), dma((envs,)), dma((envs,)), dma((envs,)),
            dma((planes, slab)), dma((planes, slab)), dma((planes, slab)), dma((planes, slab)),
            dma, dma,
        ],
        compiler_params=pltpu.CompilerParams(collective_id=0, has_side_effects=True),
        name="exchange",
    )(slot_list, held, left_env)

    bond = mpo_tensor.shape[0]
    couplings = mpo_tensor * mpo_mask.astype(jnp.float32)[:, :, None, None]
    couplings = jnp.pad(couplings, ((0, slots - bond), (0, slots - bond), (0, 0), (0, 0)))
    couplings = lax.dynamic_slice_in_dim(couplings, plane * slab, slab, 1)
    couplings = jnp.concatenate([couplings, couplings], axis=0)
    couplings = lax.dynamic_slice_in_dim(couplings, plane * slab, slots, 0)
    couplings = jnp.pad(couplings, ((0, padded - slots), (0, 0), (0, 0), (0, 0)))
    couplings = couplings.transpose(1, 2, 3, 0).reshape(slab * states, states * padded)

    chunk_rows = 64 * padded
    result = pl.pallas_call(
        functools.partial(contract_kernel, cores, pool, bond),
        out_shape=jax.ShapeDtypeStruct((slab, share, width), jnp.float32),
        in_specs=[smem, smem, smem, vmem, vmem, vmem, vmem],
        out_specs=vmem,
        scratch_shapes=[
            pltpu.SMEM((envs * cores,), jnp.int32),
            pltpu.VMEM((tiles * tile, width), jnp.float32),
            pltpu.VMEM((states, width, lanes), BF),
            pltpu.VMEM((width, tiles * tile), BF),
            pltpu.VMEM((states, chunk_rows, lanes), BF),
            pltpu.VMEM((slab, tiles * tile, lanes), BF),
        ],
        compiler_params=pltpu.CompilerParams(vmem_limit_bytes=48 * 1024 * 1024),
        name="contract",
    )(owner_map, kept, fields, arrived, left_env, other, couplings)
    return jnp.swapaxes(result, 1, 2)[:, None]


def solution(mesh):
    return jax.shard_map(
        on_device,
        mesh=mesh,
        in_specs=(
            P(("real", "env", "col"), None, None),
            P("real", None),
            P(("real", "env")),
            P("mpo", ("real", "env"), None, None),
            P(),
            P(),
            P("real"),
        ),
        out_specs=P("mpo", ("real", "env"), None, "col"),
        check_vma=False,
    )
```

```python
import functools

import jax
import jax.numpy as jnp
from jax import lax
from jax.experimental import pallas as pl
from jax.experimental.pallas import tpu as pltpu
from jax.sharding import PartitionSpec as P

MESH = pl.DeviceIdType.MESH
LANES = 128
GROUP = 4
BF = jnp.bfloat16


def iota(shape, dim):
    return lax.broadcasted_iota(jnp.int32, shape, dim)


def one_hot(condition):
    return jnp.where(condition, jnp.float32(1), jnp.float32(0)).astype(BF)


def mm(a, b):
    return jnp.dot(a, b, preferred_element_type=jnp.float32)


def list_kernel(cores, pool, map_ref, list_ref):
    rows, tiles = map_ref.shape
    low = (lax.axis_index("env") * cores + lax.axis_index("col")) * pool
    batch = 16 if tiles % 16 == 0 else 1

    def sector(t, carry):
        def step(b, count):
            found = [map_ref[t, b * batch + i] - low for i in range(batch)]
            places = [count]
            for slot in found:
                mine = (slot >= 0) & (slot < pool)
                places.append(places[-1] + mine.astype(jnp.int32))
            for slot, place in zip(found, places):
                list_ref[t, place] = slot
            return places[-1]

        lax.fori_loop(0, tiles // batch, step, jnp.int32(0))
        return carry

    lax.fori_loop(0, rows, sector, jnp.int32(0))


def quotient(value, divisor, limit):
    for shift in range(8, 31):
        factor = -(-(1 << shift) // divisor)
        if limit * factor < 2**31 and (factor * divisor - (1 << shift)) * limit < 1 << shift:
            return lax.shift_right_logical(value * factor, jnp.int32(shift))
    return lax.div(value, jnp.int32(divisor))


def comm_kernel(
    sizes, list_ref, held_ref, left_ref, arrived_ref, other_ref, pool_ref, pack_ref,
    z_send, z_recv, f_send, f_recv, x_send, x_recv, g_send, g_recv, own_sem, pool_sem,
):
    envs, planes, cores = sizes
    env, plane, core = lax.axis_index("env"), lax.axis_index("mpo"), lax.axis_index("col")
    cap = arrived_ref.shape[1]
    slab = left_ref.shape[0]
    part = left_ref.shape[2] // cores
    mate = lax.rem(core + 1, cores)

    fill = pltpu.make_async_copy(held_ref, pool_ref, pool_sem)
    fill.start()
    barrier = pltpu.get_barrier_semaphore()
    for d in range(1, envs):
        pl.semaphore_signal(
            barrier, inc=1, device_id={"env": lax.rem(env + d, envs)}, device_id_type=MESH
        )
    for d in range(1, planes):
        pl.semaphore_signal(
            barrier, inc=1, device_id={"mpo": lax.rem(plane + d, planes)}, device_id_type=MESH
        )
    pl.semaphore_signal(barrier, inc=1, device_id={"col": mate}, device_id_type=MESH)
    pl.semaphore_wait(barrier, envs + planes - 1)

    def z_copy(d):
        target = lax.rem(env + d, envs)
        return pltpu.make_async_remote_copy(
            src_ref=pack_ref.at[d],
            dst_ref=arrived_ref.at[env * cores + core],
            send_sem=z_send.at[d], recv_sem=z_recv.at[d],
            device_id={"env": target}, device_id_type=MESH,
        )

    def f_copy(d):
        source = lax.rem(env - d + envs, envs)
        block = arrived_ref.at[source * cores + core]
        return pltpu.make_async_remote_copy(
            src_ref=pack_ref.at[0] if d == 0 else block,
            dst_ref=block,
            send_sem=f_send.at[d], recv_sem=f_recv.at[d],
            device_id={"col": mate}, device_id_type=MESH,
        )

    def x_copy(d, w):
        rows = pl.ds(pl.multiple_of(core * part, part), part)
        return pltpu.make_async_remote_copy(
            src_ref=left_ref.at[w, 0, rows],
            dst_ref=other_ref.at[(planes - d - 1) * slab + w, rows],
            send_sem=x_send.at[d, w], recv_sem=x_recv.at[d, w],
            device_id={"mpo": lax.rem(plane + d, planes)}, device_id_type=MESH,
        )

    def g_copy(d, w):
        rows = pl.ds(pl.multiple_of(core * part, part), part)
        piece = other_ref.at[(planes - d - 1) * slab + w, rows]
        return pltpu.make_async_remote_copy(
            src_ref=piece, dst_ref=piece,
            send_sem=g_send.at[d, w], recv_sem=g_recv.at[d, w],
            device_id={"col": mate}, device_id_type=MESH,
        )

    own = pltpu.make_async_copy(
        pack_ref.at[0], arrived_ref.at[env * cores + core], own_sem
    )
    z_order = list(range(envs - 1, 0, -1))
    x_order = [(d, w) for w in range(slab) for d in range(1, planes)]
    for d, w in x_order:
        x_copy(d, w).start()
    fill.wait()

    def gather(d):
        target = lax.rem(env + d, envs)

        def step(p, carry):
            slot = jnp.clip(list_ref[target, p], 0, pool_ref.shape[0] - 1)
            pack_ref[d, p] = pool_ref[slot]
            return carry

        lax.fori_loop(0, cap, step, jnp.int32(0), unroll=8 if cap % 8 == 0 else 1)

    for i, d in enumerate(z_order + [0]):
        gather(d)
        if i:
            z_copy(z_order[i - 1]).start()

    waits = [("z", d, (i + 1) / len(z_order)) for i, d in enumerate(z_order)]
    waits += [("x", item, (i + 1) / len(x_order)) for i, item in enumerate(x_order)]
    own_started = False
    for kind, item, _ in sorted(waits, key=lambda entry: entry[2]):
        if kind == "z":
            z_copy(item).wait_recv()
            f_copy(item).start()
        else:
            x_copy(*item).wait_recv()
            g_copy(*item).start()
        if not own_started:
            own_started = True
            own.start()
            f_copy(0).start()
    own.wait()
    f_copy(0).wait()
    for d in z_order:
        z_copy(d).wait_send()
        f_copy(d).wait()
    for item in x_order:
        x_copy(*item).wait_send()
        g_copy(*item).wait()


def contract_kernel(
    cores, pool, bond, map_ref, kept_ref, fields_ref, arrived_ref, near_ref, far_ref, coupling_ref,
    out_ref, left_ref, other_ref, load_sem, count_ref, tiles_ref, own_ref, turned_ref, first_ref, second_ref,
):
    env, core = lax.axis_index("env"), lax.axis_index("col")
    owners, cap, tile, width = arrived_ref.shape
    tiles = map_ref.shape[1]
    states = tiles * tile // width
    slab = left_ref.shape[0]
    slots = slab + other_ref.shape[0]
    padded = coupling_ref.shape[1] // states
    share = width // cores
    lanes = own_ref.shape[2]

    loads = [
        pltpu.make_async_copy(near_ref, left_ref, load_sem.at[0]),
        pltpu.make_async_copy(far_ref, other_ref, load_sem.at[1]),
    ]
    for load in loads:
        load.start()

    for s in range(owners):
        count_ref[s] = 0

    batch = 16 if tiles % 16 == 0 else 1

    def fetch(b, carry):
        sources = [
            quotient(map_ref[env, b * batch + i], pool, pool * owners) for i in range(batch)
        ]
        ranks = []
        for source in sources:
            ranks.append(count_ref[source])
            count_ref[source] = ranks[-1] + 1
        for i in range(batch):
            at = pl.multiple_of((b * batch + i) * tile, tile)
            tiles_ref[pl.ds(at, tile), :] = arrived_ref[sources[i], ranks[i]].astype(jnp.float32)
        return carry

    lax.fori_loop(0, tiles // batch, fetch, jnp.int32(0))

    kept = kept_ref[0]
    blocks = [
        jnp.where(
            iota((width, width), 1) < kept, tiles_ref[pl.ds(s * width, width), :], 0.0
        ).astype(BF)
        for s in range(states)
    ]

    pick = one_hot(
        (iota((width, lanes), 0) == iota((width, lanes), 1) + core * share)
        & (iota((width, lanes), 1) < share)
    )
    for s in range(states):
        own_ref[s] = mm(blocks[s], pick).astype(BF)

    chunk = 256 // states
    span = chunk * states
    row, col = iota((span, span), 0), iota((span, span), 1)
    unit = states * GROUP
    moved = (
        lax.rem(lax.div(row, GROUP), states) * chunk
        + lax.div(row, unit) * GROUP
        + lax.rem(row, GROUP)
    )
    regroup = one_hot(col == moved)
    for h in range(width // chunk):
        stack = jnp.concatenate(
            [blocks[s][h * chunk : (h + 1) * chunk] for s in range(states)], axis=0
        )
        turned_ref[:, pl.ds(h * span, span)] = mm(regroup, stack).T.astype(BF)

    pairs = slab * states
    tall, wide = pairs * GROUP, states * GROUP * padded
    spread_rows = one_hot(lax.div(iota((tall, pairs), 0), GROUP) == iota((tall, pairs), 1))
    source, target = iota((states * padded, wide), 0), iota((states * padded, wide), 1)
    spread_columns = one_hot(
        (lax.div(source, padded) == lax.div(target, GROUP * padded))
        & (lax.rem(source, padded) == lax.rem(target, padded))
    )
    diagonal = lax.rem(iota((tall, wide), 0), GROUP) == lax.rem(
        lax.div(iota((tall, wide), 1), padded), GROUP
    )
    row, col = iota((pairs, states * padded), 0), iota((pairs, states * padded), 1)
    state, slot = lax.div(col, padded), lax.rem(col, padded)
    first_slot = lax.axis_index("mpo") * slab
    turn = jnp.where(first_slot + slot >= slots, slots, 0)
    corner = (
        (first_slot + lax.div(row, states) == 0)
        & (first_slot + slot - turn == bond - 1)
        & (slot < slots)
        & (lax.rem(row, states) == state)
    )
    onsite = fields_ref[0] * (0.5 - lax.div(state, 2).astype(jnp.float32)) + fields_ref[1] * (
        0.5 - lax.rem(state, 2).astype(jnp.float32)
    )
    coupling = coupling_ref[...] + jnp.where(corner, onsite, 0.0)
    high = coupling.astype(BF)
    low = (coupling - high.astype(jnp.float32)).astype(BF)
    both = []
    for piece in (high, low):
        spread = mm(mm(spread_rows, piece).astype(BF), spread_columns)
        both.append(jnp.where(diagonal, spread, 0.0).astype(BF))
    mixing = jnp.concatenate(both, axis=0)

    step = 16
    block_rows = step * padded
    row, col = iota((block_rows, block_rows), 0), iota((block_rows, block_rows), 1)
    interleave = one_hot(col == lax.rem(row, padded) * step + lax.div(row, padded))
    rows_chunk = first_ref.shape[1] // padded
    per_group = GROUP * padded

    def chunk_step(h, carry):
        pieces = []
        for b in range(rows_chunk // step):
            rows = pl.ds(pl.multiple_of(h * rows_chunk + b * step, step), step)
            stack = [left_ref[w, 0, rows, :] for w in range(slab)]
            stack += [other_ref[w, rows, :] for w in range(slots - slab)]
            if padded > slots:
                stack.append(jnp.zeros(((padded - slots) * step, width), BF))
            pieces.append(mm(interleave, jnp.concatenate(stack, axis=0)).astype(BF))
        environment = jnp.concatenate(pieces, axis=0)
        for s in range(states):
            first_ref[s] = mm(environment, own_ref[s]).astype(BF)
        for g in range(rows_chunk // GROUP):
            operand = jnp.concatenate(
                [first_ref[s, pl.ds(g * per_group, per_group), :] for s in range(states)], axis=0
            )
            mixed = mm(mixing, operand)
            mixed = (mixed[:tall] + mixed[tall:]).astype(BF)
            at = pl.multiple_of(h * (rows_chunk * states) + g * unit, unit)
            for v in range(slab):
                second_ref[v, pl.ds(at, unit), :] = mixed[v * unit : (v + 1) * unit]
        return carry

    for load in loads:
        load.wait()
    lax.fori_loop(0, width // rows_chunk, chunk_step, jnp.int32(0))

    def close(v, carry):
        out_ref[v] = mm(turned_ref[...], second_ref[v]).T[:share]
        return carry

    lax.fori_loop(0, slab, close, jnp.int32(0))


def on_device(held, owner_map, kept, left_env, mpo_tensor, mpo_mask, fields):
    envs, cores, planes = (lax.axis_size(name) for name in ("env", "col", "mpo"))
    plane = lax.axis_index("mpo")
    pool, tile, width = held.shape
    rows, tiles = owner_map.shape
    states = tiles * tile // width
    cap = 2 * kept.shape[0] * tiles // (envs * cores)
    slab = left_env.shape[0]
    slots = slab * planes
    padded = -(-slots // 16) * 16
    share = width // cores
    lanes = -(-share // LANES) * LANES
    smem = pl.BlockSpec(memory_space=pltpu.SMEM)
    vmem = pl.BlockSpec(memory_space=pltpu.VMEM)
    anywhere = pl.BlockSpec(memory_space=pl.ANY)
    dma = pltpu.SemaphoreType.DMA

    slot_list = pl.pallas_call(
        functools.partial(list_kernel, cores, pool),
        out_shape=jax.ShapeDtypeStruct((rows, cap + 1), jnp.int32),
        in_specs=[smem],
        out_specs=smem,
        name="slots",
    )(owner_map)

    arrived, other = pl.pallas_call(
        functools.partial(comm_kernel, (envs, planes, cores)),
        out_shape=[
            jax.ShapeDtypeStruct((envs * cores, cap, tile, width), BF),
            jax.ShapeDtypeStruct((slots - slab, width, width), BF),
        ],
        in_specs=[smem, anywhere, anywhere],
        out_specs=[anywhere, anywhere],
        scratch_shapes=[
            pltpu.VMEM((pool, tile, width), BF),
            pltpu.VMEM((envs, cap, tile, width), BF),
            dma((envs,)), dma((envs,)), dma((envs,)), dma((envs,)),
            dma((planes, slab)), dma((planes, slab)), dma((planes, slab)), dma((planes, slab)),
            dma, dma,
        ],
        compiler_params=pltpu.CompilerParams(collective_id=0, has_side_effects=True),
        name="exchange",
    )(slot_list, held, left_env)

    bond = mpo_tensor.shape[0]
    couplings = mpo_tensor * mpo_mask.astype(jnp.float32)[:, :, None, None]
    couplings = jnp.pad(couplings, ((0, slots - bond), (0, slots - bond), (0, 0), (0, 0)))
    couplings = lax.dynamic_slice_in_dim(couplings, plane * slab, slab, 1)
    couplings = jnp.concatenate([couplings, couplings], axis=0)
    couplings = lax.dynamic_slice_in_dim(couplings, plane * slab, slots, 0)
    couplings = jnp.pad(couplings, ((0, padded - slots), (0, 0), (0, 0), (0, 0)))
    couplings = couplings.transpose(1, 2, 3, 0).reshape(slab * states, states * padded)

    chunk_rows = 64 * padded
    result = pl.pallas_call(
        functools.partial(contract_kernel, cores, pool, bond),
        out_shape=jax.ShapeDtypeStruct((slab, share, width), jnp.float32),
        in_specs=[smem, smem, smem, vmem, anywhere, anywhere, vmem],
        out_specs=vmem,
        scratch_shapes=[
            pltpu.VMEM(left_env.shape, BF),
            pltpu.VMEM((slots - slab, width, width), BF),
            dma((2,)),
            pltpu.SMEM((envs * cores,), jnp.int32),
            pltpu.VMEM((tiles * tile, width), jnp.float32),
            pltpu.VMEM((states, width, lanes), BF),
            pltpu.VMEM((width, tiles * tile), BF),
            pltpu.VMEM((states, chunk_rows, lanes), BF),
            pltpu.VMEM((slab, tiles * tile, lanes), BF),
        ],
        compiler_params=pltpu.CompilerParams(vmem_limit_bytes=62 * 1024 * 1024),
        name="contract",
    )(owner_map, kept, fields, arrived, left_env, other, couplings)
    return jnp.swapaxes(result, 1, 2)[:, None]


def solution(mesh):
    return jax.shard_map(
        on_device,
        mesh=mesh,
        in_specs=(
            P(("real", "env", "col"), None, None),
            P("real", None),
            P(("real", "env")),
            P("mpo", ("real", "env"), None, None),
            P(),
            P(),
            P("real"),
        ),
        out_specs=P("mpo", ("real", "env"), None, "col"),
        check_vma=False,
    )
```

```python
import functools

import jax
import jax.numpy as jnp
from jax import lax
from jax.experimental import pallas as pl
from jax.experimental.pallas import tpu as pltpu
from jax.sharding import PartitionSpec as P

MESH = pl.DeviceIdType.MESH
LANES = 128
GROUP = 4
BF = jnp.bfloat16


def iota(shape, dim):
    return lax.broadcasted_iota(jnp.int32, shape, dim)


def one_hot(condition):
    return jnp.where(condition, jnp.float32(1), jnp.float32(0)).astype(BF)


def mm(a, b):
    return jnp.dot(a, b, preferred_element_type=jnp.float32)


def list_kernel(cores, pool, map_ref, list_ref):
    rows, tiles = map_ref.shape
    low = (lax.axis_index("env") * cores + lax.axis_index("col")) * pool
    batch = 16 if tiles % 16 == 0 else 1

    def sector(t, carry):
        def step(b, count):
            found = [map_ref[t, b * batch + i] - low for i in range(batch)]
            places = [count]
            for slot in found:
                mine = lax.shift_right_logical(~slot & (slot - pool), jnp.int32(31))
                places.append(places[-1] + mine)
            for slot, place in zip(found, places):
                list_ref[t, place] = slot
            return places[-1]

        lax.fori_loop(0, tiles // batch, step, jnp.int32(0))
        return carry

    lax.fori_loop(0, rows, sector, jnp.int32(0))


def quotient(value, divisor, limit):
    for shift in range(8, 31):
        factor = -(-(1 << shift) // divisor)
        if limit * factor < 2**31 and (factor * divisor - (1 << shift)) * limit < 1 << shift:
            return lax.shift_right_logical(value * factor, jnp.int32(shift))
    return lax.div(value, jnp.int32(divisor))


def comm_kernel(
    sizes, list_ref, held_ref, left_ref, arrived_ref, other_ref, pool_ref, pack_ref,
    z_send, z_recv, f_send, f_recv, x_send, x_recv, g_send, g_recv, own_sem, pool_sem,
):
    envs, planes, cores = sizes
    env, plane, core = lax.axis_index("env"), lax.axis_index("mpo"), lax.axis_index("col")
    cap = arrived_ref.shape[1]
    slab = left_ref.shape[0]
    part = left_ref.shape[2] // cores
    mate = lax.rem(core + 1, cores)

    fill = pltpu.make_async_copy(held_ref, pool_ref, pool_sem)
    fill.start()
    barrier = pltpu.get_barrier_semaphore()
    for d in range(1, envs):
        pl.semaphore_signal(
            barrier, inc=1, device_id={"env": lax.rem(env + d, envs)}, device_id_type=MESH
        )
    for d in range(1, planes):
        pl.semaphore_signal(
            barrier, inc=1, device_id={"mpo": lax.rem(plane + d, planes)}, device_id_type=MESH
        )
    pl.semaphore_signal(barrier, inc=1, device_id={"col": mate}, device_id_type=MESH)
    pl.semaphore_wait(barrier, envs + planes - 1)

    def z_copy(d):
        target = lax.rem(env + d, envs)
        return pltpu.make_async_remote_copy(
            src_ref=pack_ref.at[d],
            dst_ref=arrived_ref.at[env * cores + core],
            send_sem=z_send.at[d], recv_sem=z_recv.at[d],
            device_id={"env": target}, device_id_type=MESH,
        )

    def f_copy(d):
        source = lax.rem(env - d + envs, envs)
        block = arrived_ref.at[source * cores + core]
        return pltpu.make_async_remote_copy(
            src_ref=pack_ref.at[0] if d == 0 else block,
            dst_ref=block,
            send_sem=f_send.at[d], recv_sem=f_recv.at[d],
            device_id={"col": mate}, device_id_type=MESH,
        )

    def x_copy(d, w):
        rows = pl.ds(pl.multiple_of(core * part, part), part)
        return pltpu.make_async_remote_copy(
            src_ref=left_ref.at[w, 0, rows],
            dst_ref=other_ref.at[(planes - d - 1) * slab + w, rows],
            send_sem=x_send.at[d, w], recv_sem=x_recv.at[d, w],
            device_id={"mpo": lax.rem(plane + d, planes)}, device_id_type=MESH,
        )

    def g_copy(d, w):
        rows = pl.ds(pl.multiple_of(core * part, part), part)
        piece = other_ref.at[(planes - d - 1) * slab + w, rows]
        return pltpu.make_async_remote_copy(
            src_ref=piece, dst_ref=piece,
            send_sem=g_send.at[d, w], recv_sem=g_recv.at[d, w],
            device_id={"col": mate}, device_id_type=MESH,
        )

    own = pltpu.make_async_copy(
        pack_ref.at[0], arrived_ref.at[env * cores + core], own_sem
    )
    z_order = list(range(envs - 1, 0, -1))
    x_order = [(d, w) for w in range(slab) for d in range(1, planes)]
    for d, w in x_order:
        x_copy(d, w).start()
    fill.wait()

    def gather(d):
        target = lax.rem(env + d, envs)

        def step(p, carry):
            slot = jnp.clip(list_ref[target, p], 0, pool_ref.shape[0] - 1)
            pack_ref[d, p] = pool_ref[slot]
            return carry

        lax.fori_loop(0, cap, step, jnp.int32(0), unroll=8 if cap % 8 == 0 else 1)

    for i, d in enumerate(z_order + [0]):
        gather(d)
        if i:
            z_copy(z_order[i - 1]).start()

    waits = [("z", d, (i + 1) / len(z_order)) for i, d in enumerate(z_order)]
    waits += [("x", item, (i + 1) / len(x_order)) for i, item in enumerate(x_order)]
    own_started = False
    for kind, item, _ in sorted(waits, key=lambda entry: entry[2]):
        if kind == "z":
            z_copy(item).wait_recv()
            f_copy(item).start()
        else:
            x_copy(*item).wait_recv()
            g_copy(*item).start()
        if not own_started:
            own_started = True
            own.start()
            f_copy(0).start()
    own.wait()
    f_copy(0).wait()
    for d in z_order:
        z_copy(d).wait_send()
        f_copy(d).wait()
    for item in x_order:
        x_copy(*item).wait_send()
        g_copy(*item).wait()


def contract_kernel(
    cores, pool, bond, map_ref, kept_ref, fields_ref, arrived_ref, near_ref, far_ref, coupling_ref,
    out_ref, left_ref, other_ref, load_sem, count_ref, tiles_ref, own_ref, turned_ref, first_ref, second_ref,
):
    env, core = lax.axis_index("env"), lax.axis_index("col")
    owners, cap, tile, width = arrived_ref.shape
    tiles = map_ref.shape[1]
    states = tiles * tile // width
    slab = left_ref.shape[0]
    slots = slab + other_ref.shape[0]
    padded = coupling_ref.shape[1] // states
    share = width // cores
    lanes = own_ref.shape[2]

    loads = [
        pltpu.make_async_copy(near_ref, left_ref, load_sem.at[0]),
        pltpu.make_async_copy(far_ref, other_ref, load_sem.at[1]),
    ]
    for load in loads:
        load.start()

    for s in range(owners):
        count_ref[s] = 0

    batch = 16 if tiles % 16 == 0 else 1

    def fetch(b, carry):
        sources = [
            quotient(map_ref[env, b * batch + i], pool, pool * owners) for i in range(batch)
        ]
        ranks = []
        for source in sources:
            ranks.append(count_ref[source])
            count_ref[source] = ranks[-1] + 1
        for i in range(batch):
            at = pl.multiple_of((b * batch + i) * tile, tile)
            tiles_ref[pl.ds(at, tile), :] = arrived_ref[sources[i], ranks[i]].astype(jnp.float32)
        return carry

    lax.fori_loop(0, tiles // batch, fetch, jnp.int32(0))

    kept = kept_ref[0]
    blocks = [
        jnp.where(
            iota((width, width), 1) < kept, tiles_ref[pl.ds(s * width, width), :], 0.0
        ).astype(BF)
        for s in range(states)
    ]

    pick = one_hot(
        (iota((width, lanes), 0) == iota((width, lanes), 1) + core * share)
        & (iota((width, lanes), 1) < share)
    )
    for s in range(states):
        own_ref[s] = mm(blocks[s], pick).astype(BF)

    chunk = 256 // states
    span = chunk * states
    row, col = iota((span, span), 0), iota((span, span), 1)
    unit = states * GROUP
    moved = (
        lax.rem(lax.div(row, GROUP), states) * chunk
        + lax.div(row, unit) * GROUP
        + lax.rem(row, GROUP)
    )
    regroup = one_hot(col == moved)
    for h in range(width // chunk):
        stack = jnp.concatenate(
            [blocks[s][h * chunk : (h + 1) * chunk] for s in range(states)], axis=0
        )
        turned_ref[:, pl.ds(h * span, span)] = mm(regroup, stack).T.astype(BF)

    pairs = slab * states
    tall, wide = pairs * GROUP, states * GROUP * padded
    spread_rows = one_hot(lax.div(iota((tall, pairs), 0), GROUP) == iota((tall, pairs), 1))
    source, target = iota((states * padded, wide), 0), iota((states * padded, wide), 1)
    spread_columns = one_hot(
        (lax.div(source, padded) == lax.div(target, GROUP * padded))
        & (lax.rem(source, padded) == lax.rem(target, padded))
    )
    diagonal = lax.rem(iota((tall, wide), 0), GROUP) == lax.rem(
        lax.div(iota((tall, wide), 1), padded), GROUP
    )
    row, col = iota((pairs, states * padded), 0), iota((pairs, states * padded), 1)
    state, slot = lax.div(col, padded), lax.rem(col, padded)
    first_slot = lax.axis_index("mpo") * slab
    turn = jnp.where(first_slot + slot >= slots, slots, 0)
    corner = (
        (first_slot + lax.div(row, states) == 0)
        & (first_slot + slot - turn == bond - 1)
        & (slot < slots)
        & (lax.rem(row, states) == state)
    )
    onsite = fields_ref[0] * (0.5 - lax.div(state, 2).astype(jnp.float32)) + fields_ref[1] * (
        0.5 - lax.rem(state, 2).astype(jnp.float32)
    )
    coupling = coupling_ref[...] + jnp.where(corner, onsite, 0.0)
    high = coupling.astype(BF)
    low = (coupling - high.astype(jnp.float32)).astype(BF)
    both = []
    for piece in (high, low):
        spread = mm(mm(spread_rows, piece).astype(BF), spread_columns)
        both.append(jnp.where(diagonal, spread, 0.0).astype(BF))
    mixing = jnp.concatenate(both, axis=0)

    step = 16
    block_rows = step * padded
    row, col = iota((block_rows, block_rows), 0), iota((block_rows, block_rows), 1)
    interleave = one_hot(col == lax.rem(row, padded) * step + lax.div(row, padded))
    rows_chunk = first_ref.shape[1] // padded
    per_group = GROUP * padded

    def chunk_step(h, carry):
        pieces = []
        for b in range(rows_chunk // step):
            rows = pl.ds(pl.multiple_of(h * rows_chunk + b * step, step), step)
            stack = [left_ref[w, 0, rows, :] for w in range(slab)]
            stack += [other_ref[w, rows, :] for w in range(slots - slab)]
            if padded > slots:
                stack.append(jnp.zeros(((padded - slots) * step, width), BF))
            pieces.append(mm(interleave, jnp.concatenate(stack, axis=0)).astype(BF))
        environment = jnp.concatenate(pieces, axis=0)
        for s in range(states):
            first_ref[s] = mm(environment, own_ref[s]).astype(BF)
        for g in range(rows_chunk // GROUP):
            operand = jnp.concatenate(
                [first_ref[s, pl.ds(g * per_group, per_group), :] for s in range(states)], axis=0
            )
            mixed = mm(mixing, operand)
            mixed = (mixed[:tall] + mixed[tall:]).astype(BF)
            at = pl.multiple_of(h * (rows_chunk * states) + g * unit, unit)
            for v in range(slab):
                second_ref[v, pl.ds(at, unit), :] = mixed[v * unit : (v + 1) * unit]
        return carry

    for load in loads:
        load.wait()
    lax.fori_loop(0, width // rows_chunk, chunk_step, jnp.int32(0))

    def close(v, carry):
        out_ref[v] = mm(turned_ref[...], second_ref[v]).T[:share]
        return carry

    lax.fori_loop(0, slab, close, jnp.int32(0))


def on_device(held, owner_map, kept, left_env, mpo_tensor, mpo_mask, fields):
    envs, cores, planes = (lax.axis_size(name) for name in ("env", "col", "mpo"))
    plane = lax.axis_index("mpo")
    pool, tile, width = held.shape
    rows, tiles = owner_map.shape
    states = tiles * tile // width
    cap = 2 * kept.shape[0] * tiles // (envs * cores)
    slab = left_env.shape[0]
    slots = slab * planes
    padded = -(-slots // 16) * 16
    share = width // cores
    lanes = -(-share // LANES) * LANES
    smem = pl.BlockSpec(memory_space=pltpu.SMEM)
    vmem = pl.BlockSpec(memory_space=pltpu.VMEM)
    anywhere = pl.BlockSpec(memory_space=pl.ANY)
    dma = pltpu.SemaphoreType.DMA

    slot_list = pl.pallas_call(
        functools.partial(list_kernel, cores, pool),
        out_shape=jax.ShapeDtypeStruct((rows, cap + 1), jnp.int32),
        in_specs=[smem],
        out_specs=smem,
        name="slots",
    )(owner_map)

    arrived, other = pl.pallas_call(
        functools.partial(comm_kernel, (envs, planes, cores)),
        out_shape=[
            jax.ShapeDtypeStruct((envs * cores, cap, tile, width), BF),
            jax.ShapeDtypeStruct((slots - slab, width, width), BF),
        ],
        in_specs=[smem, anywhere, anywhere],
        out_specs=[anywhere, anywhere],
        scratch_shapes=[
            pltpu.VMEM((pool, tile, width), BF),
            pltpu.VMEM((envs, cap, tile, width), BF),
            dma((envs,)), dma((envs,)), dma((envs,)), dma((envs,)),
            dma((planes, slab)), dma((planes, slab)), dma((planes, slab)), dma((planes, slab)),
            dma, dma,
        ],
        compiler_params=pltpu.CompilerParams(collective_id=0, has_side_effects=True),
        name="exchange",
    )(slot_list, held, left_env)

    bond = mpo_tensor.shape[0]
    couplings = mpo_tensor * mpo_mask.astype(jnp.float32)[:, :, None, None]
    couplings = jnp.pad(couplings, ((0, slots - bond), (0, slots - bond), (0, 0), (0, 0)))
    couplings = lax.dynamic_slice_in_dim(couplings, plane * slab, slab, 1)
    couplings = jnp.concatenate([couplings, couplings], axis=0)
    couplings = lax.dynamic_slice_in_dim(couplings, plane * slab, slots, 0)
    couplings = jnp.pad(couplings, ((0, padded - slots), (0, 0), (0, 0), (0, 0)))
    couplings = couplings.transpose(1, 2, 3, 0).reshape(slab * states, states * padded)

    chunk_rows = 64 * padded
    result = pl.pallas_call(
        functools.partial(contract_kernel, cores, pool, bond),
        out_shape=jax.ShapeDtypeStruct((slab, share, width), jnp.float32),
        in_specs=[smem, smem, smem, vmem, anywhere, anywhere, vmem],
        out_specs=vmem,
        scratch_shapes=[
            pltpu.VMEM(left_env.shape, BF),
            pltpu.VMEM((slots - slab, width, width), BF),
            dma((2,)),
            pltpu.SMEM((envs * cores,), jnp.int32),
            pltpu.VMEM((tiles * tile, width), jnp.float32),
            pltpu.VMEM((states, width, lanes), BF),
            pltpu.VMEM((width, tiles * tile), BF),
            pltpu.VMEM((states, chunk_rows, lanes), BF),
            pltpu.VMEM((slab, tiles * tile, lanes), BF),
        ],
        compiler_params=pltpu.CompilerParams(vmem_limit_bytes=62 * 1024 * 1024),
        name="contract",
    )(owner_map, kept, fields, arrived, left_env, other, couplings)
    return jnp.swapaxes(result, 1, 2)[:, None]


def solution(mesh):
    return jax.shard_map(
        on_device,
        mesh=mesh,
        in_specs=(
            P(("real", "env", "col"), None, None),
            P("real", None),
            P(("real", "env")),
            P("mpo", ("real", "env"), None, None),
            P(),
            P(),
            P("real"),
        ),
        out_specs=P("mpo", ("real", "env"), None, "col"),
        check_vma=False,
    )
```
